32 devices in a mesh: dp: 8 (over y, x, core), feat: 4 (over z).
Axes of the slice: x: 2, y: 2, z: 4, core: 2. Of those that a mesh axis runs over, the one named last changes fastest.
Arguments:
- hidden_states: bfloat16 [64, 256, 1152], P(('dp', 'feat')), may hold values from -6 to 6
- teacher: bfloat16 [64, 256, 1024], P('dp', None, 'feat'), may hold values from -6 to 6
- proj_in: bfloat16 [2048, 1152], replicated, may hold values from -0.1875 to 0.1875
- bias_in: float32 [2048], replicated, may hold values from -3 to 3
- proj_out: bfloat16 [2048, 1024], replicated, may hold values from -0.125 to 0.125
- bias_out: float32 [1024], replicated, may hold values from -3 to 3
Outputs:
- grad_proj_in: float32 [2048, 1152], P(('dp', 'feat'))
- grad_bias_in: float32 [2048], P(('dp', 'feat'))
- grad_proj_out: float32 [2048, 1024], P(('dp', 'feat'))
- grad_bias_out: float32 [1024], replicated
- grad_hidden: bfloat16 [64, 256, 1152], P(('dp', 'feat'))
- loss: float32 [], replicated
The draws below stay inside these ranges and needn't reach their ends.
All inputs are finite; a program needn't handle non-finite values.
Results may differ from the reference program's by a relative error of at most 0.0095.
The reference program's roundings to bfloat16 on the way (of `act`, `cot` and `dpre`) count: a program that leaves them out, or rounds other values in their place, can miss the bound.
Values may be sent and summed in bfloat16 or wider, within the bound.
A program may use at most 128 MiB of HBM per device.

```python
import jax
import jax.numpy as jnp
from jax import lax

D = 1152
H = 2048
E = 1024
L = 256
B_DEV = 2
BATCH = 64
N_FEAT = 4


def levels(own_key, shape, shards, smallest, top_value):
    def one(position, shards_of):
        draws = jax.random.uniform(jax.random.fold_in(jax.random.fold_in(own_key, 6), position), (shards_of,), jnp.float32, smallest / len(shards), top_value / len(shards))
        return jnp.repeat(jnp.exp(draws), shape[position] // shards_of).reshape((-1,) + (1,) * (len(shape) - position - 1))

    level = one(*shards[0])
    for cut in shards[1:]:
        level = level * one(*cut)
    return level


def gaussian(key, extent, deviation, bound, cuts=(), dtype=jnp.bfloat16):
    result = jax.random.normal(key, extent, jnp.float32) * deviation
    if len(cuts) > 0:
        result = levels(key, extent, cuts, -0.22, 0.18) * result
    return jnp.clip(result, min=-bound, max=bound).astype(dtype)


def setup_inputs(seed: int = 0) -> dict:
    streams_of = jax.random.split(jax.random.key(seed), 7)
    hidden_states = gaussian(streams_of[0], (BATCH, L, D), 1.0, 6.0, ((0, 32),))
    teacher = gaussian(streams_of[1], (BATCH, L, E), 1.0, 6.0, ((0, 8), (2, 4)))
    proj_in = gaussian(streams_of[2], (H, D), D ** -0.5, 0.1875)
    bias_in = gaussian(streams_of[3], (H,), 0.5, 3.0, (), jnp.float32)
    proj_out = gaussian(streams_of[4], (H, E), H ** -0.5, 0.125)
    bias_out = gaussian(streams_of[5], (E,), 0.5, 3.0, (), jnp.float32)
    return {"hidden_states": hidden_states, "teacher": teacher, "proj_in": proj_in, "bias_in": bias_in, "proj_out": proj_out, "bias_out": bias_out}


epsilon = 1e-06

def reference(hidden_states, teacher, proj_in, bias_in, proj_out, bias_out):
    scale = 1.0 / float(BATCH * L)
    group = B_DEV * N_FEAT
    blocks = BATCH // group
    hid_blocks = hidden_states.reshape(blocks, group * L, D)
    tea_blocks = teacher.reshape(blocks, group * L, E)

    def step(carry, items):
        rows, target_raw = items
        g_in, b_in, g_out, b_out, loss_sum = carry
        pre = lax.dot_general(rows, proj_in, (((1,), (1,)), ((), ())), preferred_element_type=jnp.float32) + bias_in
        act = jax.nn.silu(pre).astype(jnp.bfloat16)
        out = jnp.dot(act, proj_out, preferred_element_type=jnp.float32) + bias_out
        target = target_raw.astype(jnp.float32)
        zz = lax.optimization_barrier(jnp.sum(out * out, axis=1))
        yy = lax.optimization_barrier(jnp.sum(target * target, axis=1))
        zy = lax.optimization_barrier(jnp.sum(out * target, axis=1))
        norm_z = jnp.sqrt(zz + epsilon)
        norm_y = jnp.sqrt(yy + epsilon)
        cosine = zy / (norm_z * norm_y)
        cot = (-(target / (norm_z * norm_y)[:, None] - (cosine / (norm_z * norm_z))[:, None] * out)).astype(jnp.bfloat16)
        back = lax.dot_general(cot, proj_out, (((1,), (1,)), ((), ())), preferred_element_type=jnp.float32)
        sig = jax.nn.sigmoid(pre)
        dpre = (back * sig * (1.0 + pre * (1.0 - sig))).astype(jnp.bfloat16)
        g_out = g_out + lax.dot_general(act, cot, (((0,), (0,)), ((), ())), preferred_element_type=jnp.float32)
        b_out = b_out + lax.optimization_barrier(jnp.sum(cot.astype(jnp.float32), axis=0))
        g_in = g_in + lax.dot_general(dpre, rows, (((0,), (0,)), ((), ())), preferred_element_type=jnp.float32)
        b_in = b_in + lax.optimization_barrier(jnp.sum(dpre.astype(jnp.float32), axis=0))
        loss_sum = loss_sum + jnp.sum(cosine)
        grad_rows = jnp.dot(dpre, proj_in, preferred_element_type=jnp.float32).astype(jnp.bfloat16)
        return ((g_in, b_in, g_out, b_out, loss_sum), grad_rows)
    init = (jnp.zeros((H, D), jnp.float32), jnp.zeros((H,), jnp.float32), jnp.zeros((H, E), jnp.float32), jnp.zeros((E,), jnp.float32), jnp.zeros((), jnp.float32))
    carry, grad_rows = lax.scan(step, init, (hid_blocks, tea_blocks))
    g_in, b_in, g_out, b_out, loss_sum = carry
    return (g_in * scale, b_in * scale, g_out * scale, b_out * scale, grad_rows.reshape(BATCH, L, D), -loss_sum * scale)
```

```python
import functools

import jax
import jax.numpy as jnp
from jax import lax
from jax.experimental import pallas as pl
from jax.experimental.pallas import tpu as pltpu
from jax.sharding import PartitionSpec as P

epsilon = 1e-06
f32 = jnp.float32
bf16 = jnp.bfloat16


def log2(n):
    return n.bit_length() - 1


def stage_orders(dp, feat):
    m, f = log2(dp), log2(feat)
    across = [("dp", b) for b in range(1, m)]
    half = len(across) // 2
    tail = [("feat", b) for b in range(f)]
    first = [("dp", 0)] + across + tail
    second = [("dp", 0)] + across[half:] + across[:half] + tail
    return first, second


def splits(order, dp, feat):
    left = [("dp", b) for b in reversed(range(log2(dp)))] + [("feat", b) for b in reversed(range(log2(feat)))]
    out = []
    for bit in order:
        p = left.index(bit)
        out.append((2**p, 2 ** (len(left) - p - 1)))
        left.remove(bit)
    return out


def grads_kernel(plan, scale, act, cot, dpre, rows, small, gout, gin, gsmall, act_t, dpre_t, *rest):
    streams, dp, feat, blk = plan
    stages = log2(dp) + log2(feat)
    per = 3 * stages
    bufs = [rest[i * per : (i + 1) * per] for i in range(len(streams))]
    small_send, small_recv, send_sem, recv_sem = rest[len(streams) * per :]
    place = {"dp": lax.axis_index("dp"), "feat": lax.axis_index("feat")}

    def mine(bit):
        axis, b = bit
        return lax.rem(lax.div(place[axis], 2**b), 2)

    def partner(bit):
        axis, b = bit
        return {axis: place[axis] + (1 - 2 * mine(bit)) * 2**b}

    barrier = pltpu.get_barrier_semaphore()
    for bit in streams[0][0]:
        pl.semaphore_signal(barrier, inc=1, device_id=partner(bit), device_id_type=pl.DeviceIdType.MESH)
    pl.semaphore_wait(barrier, stages)

    def copy(s, k):
        keep, send, recv = bufs[s][3 * k : 3 * k + 3]
        return pltpu.make_async_remote_copy(
            src_ref=send, dst_ref=recv, send_sem=send_sem.at[s, k], recv_sem=recv_sem.at[s, k],
            device_id=partner(streams[s][0][k]), device_id_type=pl.DeviceIdType.MESH,
        )

    def small_copy(k):
        return pltpu.make_async_remote_copy(
            src_ref=small_send.at[k], dst_ref=small_recv.at[k],
            send_sem=send_sem.at[len(streams), k], recv_sem=recv_sem.at[len(streams), k],
            device_id=partner(streams[0][0][k]), device_id_type=pl.DeviceIdType.MESH,
        )

    def transpose(source, target):
        wide = min(256, source.shape[1])

        def body(j, _):
            at = pl.multiple_of(j * wide, wide)
            target[pl.ds(at, wide), :] = source[:, pl.ds(at, wide)].T
            return 0

        lax.fori_loop(0, source.shape[1] // wide, body, 0)

    def produce(s):
        order, split, which, lo_col, hi_col = streams[s]
        lhs, rhs = (act_t, cot) if which == 0 else (dpre_t, rows)
        hi, lo = split[0]
        keep, send, recv = bufs[s][:3]
        own = mine(order[0])

        def term(h, bit):
            at = pl.multiple_of((h * 2 + bit) * (lo * blk), lo * blk)
            got = jnp.dot(lhs[pl.ds(at, lo * blk), :], rhs[:, lo_col:hi_col], preferred_element_type=f32)
            return got.reshape(lo, blk, hi_col - lo_col)

        def to_send(h, _):
            send[pl.ds(h * lo, lo)] = term(h, 1 - own).astype(bf16)
            return 0

        def to_keep(h, _):
            keep[pl.ds(h * lo, lo)] = term(h, own)
            return 0

        lax.fori_loop(0, hi, to_send, 0)
        copy(s, 0).start()
        lax.fori_loop(0, hi, to_keep, 0)

    def advance(s, k):
        order, split = streams[s][:2]
        hi, lo = split[k]
        keep0, _, recv0 = bufs[s][3 * k - 3 : 3 * k]
        keep, send, recv = bufs[s][3 * k : 3 * k + 3]
        own = mine(order[k])
        copy(s, k - 1).wait_recv()

        def total(i, bit):
            at = (lax.div(i, lo) * 2 + bit) * lo + lax.rem(i, lo)
            return keep0[at] + recv0[at].astype(f32)

        def to_send(i, _):
            send[i] = total(i, 1 - own).astype(bf16)
            return 0

        def to_keep(i, _):
            keep[i] = total(i, own)
            return 0

        lax.fori_loop(0, hi * lo, to_send, 0)
        copy(s, k).start()
        lax.fori_loop(0, hi * lo, to_keep, 0)

    def small_step(k):
        if k == 0:
            small_send[0] = small[...]
        else:
            small_copy(k - 1).wait_recv()
            small_send[k] = small_send[k - 1] + small_recv[k - 1]
        small_copy(k).start()

    def finish(s):
        order, split, which, lo_col, hi_col = streams[s]
        keep, _, recv = bufs[s][3 * stages - 3 :]
        copy(s, stages - 1).wait_recv()
        out = gout if which == 0 else gin
        out[:, lo_col:hi_col] = (keep[0] + recv[0].astype(f32)) * scale

    half = len(streams) // 2
    early, late = range(half), range(half, len(streams))
    transpose(act, act_t)
    for s in early:
        produce(s)
    small_step(0)
    for t in range(1, stages + 2):
        for s in early:
            if t < stages:
                advance(s, t)
            elif t == stages:
                finish(s)
        if t < stages:
            small_step(t)
        if t == 1:
            transpose(dpre, dpre_t)
            for s in late:
                produce(s)
        elif t <= stages:
            for s in late:
                advance(s, t - 1)
        else:
            for s in late:
                finish(s)
    small_copy(stages - 1).wait_recv()
    gsmall[...] = (small_send[stages - 1] + small_recv[stages - 1]) * scale
    for k in range(stages):
        for s in range(len(streams)):
            copy(s, k).wait_send()
        small_copy(k).wait_send()


def reduce_grads(act, cot, dpre, rows, small, scale, dp, feat):
    tokens, hidden = act.shape
    channels, width = cot.shape[1], rows.shape[1]
    blk = hidden // (dp * feat)
    orders = stage_orders(dp, feat)
    stages = log2(dp) + log2(feat)
    streams, bufs = [], []
    for which, size in ((0, channels), (1, width)):
        cut = (size // 2 + 127) // 128 * 128
        for order, lo, hi in ((orders[0], 0, cut), (orders[1], cut, size)):
            split = splits(order, dp, feat)
            streams.append((order, split, which, lo, hi))
            for above, below in split:
                shape = (above * below, blk, hi - lo)
                bufs += [pltpu.VMEM(shape, f32), pltpu.VMEM(shape, bf16), pltpu.VMEM(shape, bf16)]
    vmem = pl.BlockSpec(memory_space=pltpu.VMEM)
    return pl.pallas_call(
        functools.partial(grads_kernel, (streams, dp, feat, blk), scale),
        out_shape=(
            jax.ShapeDtypeStruct((blk, channels), f32),
            jax.ShapeDtypeStruct((blk, width), f32),
            jax.ShapeDtypeStruct(small.shape, f32),
        ),
        in_specs=[vmem] * 5,
        out_specs=(vmem,) * 3,
        scratch_shapes=[pltpu.VMEM((hidden, tokens), bf16), pltpu.VMEM((hidden, tokens), bf16)]
        + bufs
        + [
            pltpu.VMEM((stages,) + small.shape, f32),
            pltpu.VMEM((stages,) + small.shape, f32),
            pltpu.SemaphoreType.DMA((len(streams) + 1, stages)),
            pltpu.SemaphoreType.DMA((len(streams) + 1, stages)),
        ],
        compiler_params=pltpu.CompilerParams(collective_id=0, has_side_effects=True, vmem_limit_bytes=60 * 1024 * 1024),
        name="grads",
    )(act, cot, dpre, rows, small)


def on_device(hidden_states, teacher, proj_in, bias_in, proj_out, bias_out):
    samples, seq, width = hidden_states.shape
    hidden, channels = proj_out.shape
    rows = hidden_states.reshape(samples * seq, width)
    dp, feat = lax.axis_size("dp"), lax.axis_size("feat")
    scale = 1.0 / float(samples * seq * dp * feat)
    target = lax.all_to_all(teacher, "feat", split_axis=0, concat_axis=2, tiled=True)
    target = target.reshape(samples * seq, channels).astype(f32)
    pre = lax.dot_general(rows, proj_in, (((1,), (1,)), ((), ())), preferred_element_type=f32) + bias_in
    act = jax.nn.silu(pre).astype(bf16)
    out = jnp.dot(act, proj_out, preferred_element_type=f32) + bias_out
    zz = jnp.sum(out * out, axis=1)
    yy = jnp.sum(target * target, axis=1)
    zy = jnp.sum(out * target, axis=1)
    norm_z = jnp.sqrt(zz + epsilon)
    norm_y = jnp.sqrt(yy + epsilon)
    cosine = zy / (norm_z * norm_y)
    cot = (-(target / (norm_z * norm_y)[:, None] - (cosine / (norm_z * norm_z))[:, None] * out)).astype(bf16)
    back = lax.dot_general(cot, proj_out, (((1,), (1,)), ((), ())), preferred_element_type=f32)
    sig = jax.nn.sigmoid(pre)
    dpre = (back * sig * (1.0 + pre * (1.0 - sig))).astype(bf16)
    grad_hidden = jnp.dot(dpre, proj_in, preferred_element_type=f32).astype(bf16).reshape(samples, seq, width)
    parts = [jnp.sum(dpre.astype(f32), axis=0), jnp.sum(cot.astype(f32), axis=0), jnp.sum(cosine)[None]]
    count = hidden + channels + 1
    padded = -(-count // 1024) * 1024
    small = jnp.concatenate(parts + [jnp.zeros((padded - count,), f32)]).reshape(padded // 128, 128)
    gout, gin, sums = reduce_grads(act, cot, dpre, rows, small, scale, dp, feat)
    sums = sums.reshape(padded)
    blk = hidden // (dp * feat)
    me = lax.axis_index("dp") * feat + lax.axis_index("feat")
    return (
        gin,
        lax.dynamic_slice(sums, (me * blk,), (blk,)),
        gout,
        sums[hidden : hidden + channels],
        grad_hidden,
        -sums[hidden + channels],
    )


def solution(mesh):
    return jax.shard_map(
        on_device,
        mesh=mesh,
        in_specs=(P(("dp", "feat"), None, None), P("dp", None, "feat"), P(), P(), P(), P()),
        out_specs=(
            P(("dp", "feat"), None),
            P(("dp", "feat")),
            P(("dp", "feat"), None),
            P(),
            P(("dp", "feat"), None, None),
            P(),
        ),
        check_vma=False,
    )
```

```python
import functools

import jax
import jax.numpy as jnp
from jax import lax
from jax.experimental import pallas as pl
from jax.experimental.pallas import tpu as pltpu
from jax.sharding import PartitionSpec as P

epsilon = 1e-06
f32 = jnp.float32
bf16 = jnp.bfloat16
MESH = pl.DeviceIdType.MESH


def log2(n):
    return n.bit_length() - 1


def stage_orders(dp, feat):
    across = [("dp", b) for b in range(1, log2(dp))]
    along = [("feat", b) for b in range(log2(feat))]
    half = len(across) // 2
    core = [("dp", 0)]
    return core + across + along, core + across[half:] + across[:half] + along, core + along + across


def splits(order, dp, feat):
    left = [("dp", b) for b in reversed(range(log2(dp)))] + [("feat", b) for b in reversed(range(log2(feat)))]
    out = []
    for bit in order:
        p = left.index(bit)
        out.append((2**p, 2 ** (len(left) - p - 1)))
        left.remove(bit)
    return out


def train_kernel(plan, teacher_hbm, rows_hbm, win_hbm, wout_hbm, bias_in, bias_out, gout, gin, gsmall, ghid,
                 rows, win, wout, tea, act, act_t, dpre_t, dsilu, out, cot, brow, bacc, lacc, *rest):
    groups, streams, dp, feat, blk = plan
    stages = log2(dp) + log2(feat)
    bufs, at = [], 0
    for _ in streams:
        bufs.append(rest[at : at + 1 + 2 * stages])
        at += 1 + 2 * stages
    small_send, small_recv, send_sem, recv_sem, tea_send, tea_recv, load_sem = rest[at:]
    place = {"dp": lax.axis_index("dp"), "feat": lax.axis_index("feat")}
    dpre = act
    tokens, hidden = act.shape
    channels, width = cot.shape[1], rows.shape[1]
    samples, seq, part = tea.shape[1:]

    def mine(bit):
        axis, b = bit
        return lax.rem(lax.div(place[axis], 2**b), 2)

    def partner(bit):
        axis, b = bit
        return {axis: place[axis] + (1 - 2 * mine(bit)) * 2**b}

    barrier = pltpu.get_barrier_semaphore()
    for b in range(log2(dp)):
        pl.semaphore_signal(barrier, inc=1, device_id=partner(("dp", b)), device_id_type=MESH)
    for r in range(1, feat):
        peer = {"feat": lax.rem(place["feat"] + r, feat)}
        pl.semaphore_signal(barrier, inc=1, device_id=peer, device_id_type=MESH)

    loads = [
        pltpu.make_async_copy(rows_hbm, rows, load_sem.at[0]),
        pltpu.make_async_copy(win_hbm, win, load_sem.at[1]),
        pltpu.make_async_copy(wout_hbm, wout, load_sem.at[2]),
        pltpu.make_async_copy(
            teacher_hbm.at[pl.ds(place["feat"] * samples, samples)], tea.at[place["feat"]], load_sem.at[3]
        ),
    ]
    for load in loads:
        load.start()
    pl.semaphore_wait(barrier, log2(dp) + feat - 1)

    def tea_copy(r):
        peer = lax.rem(place["feat"] + r, feat)
        return pltpu.make_async_remote_copy(
            src_ref=teacher_hbm.at[pl.ds(peer * samples, samples)], dst_ref=tea.at[place["feat"]],
            send_sem=tea_send.at[r - 1], recv_sem=tea_recv.at[r - 1],
            device_id={"feat": peer}, device_id_type=MESH,
        )

    for r in range(1, feat):
        tea_copy(r).start()

    def copy(s, k):
        send, recv = bufs[s][1 + 2 * k : 3 + 2 * k]
        return pltpu.make_async_remote_copy(
            src_ref=send, dst_ref=recv, send_sem=send_sem.at[s, k], recv_sem=recv_sem.at[s, k],
            device_id=partner(streams[s][0][k]), device_id_type=MESH,
        )

    def small_copy(k):
        return pltpu.make_async_remote_copy(
            src_ref=small_send.at[k], dst_ref=small_recv.at[k],
            send_sem=send_sem.at[len(streams), k], recv_sem=recv_sem.at[len(streams), k],
            device_id=partner(streams[0][0][k]), device_id_type=MESH,
        )

    wide = 256

    def first_map(j, _):
        cut = pl.ds(pl.multiple_of(j * wide, wide), wide)
        pre = lax.dot_general(rows[...], win[cut, :], (((1,), (1,)), ((), ())), preferred_element_type=f32)
        pre = pre + bias_in[:, cut]
        sig = jax.nn.sigmoid(pre)
        got = (pre * sig).astype(bf16)
        act[:, cut] = got
        act_t[cut, :] = got.T
        dsilu[:, cut] = sig * (1.0 + pre * (1.0 - sig))
        return 0

    def last_map(j, _):
        cut = pl.ds(pl.multiple_of(j * wide, wide), wide)
        out[:, cut] = jnp.dot(act[...], wout[:, cut], preferred_element_type=f32) + bias_out[:, cut]
        return 0

    some = 64

    def cotangent(i, loss):
        at = pl.ds(pl.multiple_of(i * some, some), some)
        sample, off = lax.div(i, seq // some), lax.rem(i, seq // some)
        inner = pl.ds(pl.multiple_of(off * some, some), some)
        zz = jnp.zeros((some, 1), f32)
        yy, zy = zz, zz
        for c in range(feat):
            o = out[at, c * part : (c + 1) * part]
            t = tea[c, sample, inner, :].astype(f32)
            zz = zz + jnp.sum(o * o, axis=1, keepdims=True)
            yy = yy + jnp.sum(t * t, axis=1, keepdims=True)
            zy = zy + jnp.sum(o * t, axis=1, keepdims=True)
        norm_z = jnp.sqrt(zz + epsilon)
        norm_y = jnp.sqrt(yy + epsilon)
        inverse = 1.0 / (norm_z * norm_y)
        cosine = zy * inverse
        weight = cosine / (norm_z * norm_z)
        for c in range(feat):
            o = out[at, c * part : (c + 1) * part]
            t = tea[c, sample, inner, :].astype(f32)
            got = (weight * o - t * inverse).astype(bf16)
            cot[at, c * part : (c + 1) * part] = got
            bacc[:, c * part : (c + 1) * part] += jnp.sum(got.astype(f32), axis=0, keepdims=True)
        return loss + jnp.sum(cosine, axis=0, keepdims=True)

    def backward(j, _):
        cut = pl.ds(pl.multiple_of(j * wide, wide), wide)
        back = lax.dot_general(cot[...], wout[cut, :], (((1,), (1,)), ((), ())), preferred_element_type=f32)
        got = (back * dsilu[:, cut]).astype(bf16)
        dpre[:, cut] = got
        dpre_t[cut, :] = got.T
        brow[:, cut] = jnp.sum(got.astype(f32), axis=0, keepdims=True)
        return 0

    step = 384 if width % 384 == 0 else 128

    def to_rows(j, _):
        cut = pl.ds(pl.multiple_of(j * step, step), step)
        ghid[:, cut] = jnp.dot(dpre[...], win[:, cut], preferred_element_type=f32).astype(bf16)
        return 0

    def produce(s):
        order, split, which, lo_col, hi_col = streams[s]
        lhs, rhs = (act_t, cot) if which == 0 else (dpre_t, rows)
        hi, lo = split[0]
        keep, send, recv = bufs[s][:3]
        own = mine(order[0])

        def term(h, bit):
            at = pl.multiple_of((h * 2 + bit) * (lo * blk), lo * blk)
            got = jnp.dot(lhs[pl.ds(at, lo * blk), :], rhs[:, lo_col:hi_col], preferred_element_type=f32)
            return got.reshape(lo, blk, hi_col - lo_col)

        def to_send(h, _):
            send[pl.ds(h * lo, lo)] = term(h, 1 - own).astype(bf16)
            return 0

        def to_keep(h, _):
            keep[pl.ds(h * lo, lo)] = term(h, own)
            return 0

        lax.fori_loop(0, hi, to_send, 0)
        copy(s, 0).start()
        lax.fori_loop(0, hi, to_keep, 0)

    def advance(s, k):
        order, split = streams[s][:2]
        hi, lo = split[k]
        keep, recv0, send = bufs[s][0], bufs[s][2 * k], bufs[s][2 * k + 1]
        own = mine(order[k])
        copy(s, k - 1).wait_recv()

        def total(i, bit):
            at = (lax.div(i, lo) * 2 + bit) * lo + lax.rem(i, lo)
            return keep[at] + recv0[at].astype(f32)

        def to_send(i, _):
            send[i] = total(i, 1 - own).astype(bf16)
            return 0

        def to_keep(i, _):
            keep[i] = total(i, own)
            return 0

        lax.fori_loop(0, hi * lo, to_send, 0)
        copy(s, k).start()
        lax.fori_loop(0, hi * lo, to_keep, 0)

    blocks = dp * feat

    def small_step(k):
        if k == 0:
            small_send[0] = jnp.zeros(small_send.shape[1:], f32)
            for j in range(blocks):
                small_send[0, j : j + 1, 0:blk] = brow[:, j * blk : (j + 1) * blk]
            for j in range(channels // 128):
                small_send[0, blocks + j : blocks + j + 1, :] = bacc[:, j * 128 : (j + 1) * 128]
            last = blocks + channels // 128
            small_send[0, last : last + 1, :] = jnp.broadcast_to(lacc[...], (1, 128))
        else:
            small_copy(k - 1).wait_recv()
            small_send[k] = small_send[k - 1] + small_recv[k - 1]
        small_copy(k).start()

    def finish(s):
        which, lo_col, hi_col = streams[s][2:]
        copy(s, stages - 1).wait_recv()
        target = gout if which == 0 else gin
        target[:, lo_col:hi_col] = bufs[s][0][0] + bufs[s][2 * stages][0].astype(f32)

    loads[0].wait()
    loads[1].wait()
    lax.fori_loop(0, hidden // wide, first_map, 0)
    loads[2].wait()
    lax.fori_loop(0, channels // wide, last_map, 0)
    bacc[...] = jnp.zeros_like(bacc)
    loads[3].wait()
    for r in range(1, feat):
        tea_copy(r).wait_recv()
    lacc[...] = lax.fori_loop(0, tokens // some, cotangent, jnp.zeros((1, 1), f32))

    for t in range(stages + len(groups)):
        for g, group in enumerate(groups):
            k = t - g
            for s in group:
                if k == 0:
                    produce(s)
                elif 0 < k < stages:
                    advance(s, k)
                elif k == stages:
                    finish(s)
            if t == 1 and g == 0:
                lax.fori_loop(0, hidden // wide, backward, 0)
            if g == 1 and 0 <= k < stages:
                small_step(k)
        if t == 2:
            lax.fori_loop(0, width // step, to_rows, 0)
    small_copy(stages - 1).wait_recv()
    gsmall[...] = small_send[stages - 1] + small_recv[stages - 1]
    for r in range(1, feat):
        tea_copy(r).wait_send()
    for k in range(stages):
        for s in range(len(streams)):
            copy(s, k).wait_send()
        small_copy(k).wait_send()


def place_kernel(scale, blocks, gout, gin, gsmall, ghid, out_in, out_bias_in, out_out, out_bias_out, out_hid, out_loss):
    me = lax.axis_index("dp") * lax.axis_size("feat") + lax.axis_index("feat")
    out_in[...] = gin[...] * scale
    out_out[...] = gout[...] * scale
    out_hid[...] = ghid[...]
    blk = out_bias_in.shape[1]
    out_bias_in[...] = gsmall[pl.ds(me, 1), 0:blk] * scale
    rows = out_bias_out.shape[0]
    out_bias_out[...] = gsmall[blocks : blocks + rows, :] * scale
    out_loss[...] = gsmall[blocks + rows : blocks + rows + 1, 0:1] * (-scale)


def units(size, shares):
    total, parts, edge = size // 128, [], 0
    for i in range(len(shares)):
        upto = round(total * sum(shares[: i + 1]) / sum(shares))
        parts.append((edge * 128, upto * 128 if i < len(shares) - 1 else size))
        edge = upto
    return parts


def on_device(hidden_states, teacher, proj_in, bias_in, proj_out, bias_out):
    samples, seq, width = hidden_states.shape
    hidden, channels = proj_out.shape
    tokens = samples * seq
    rows = hidden_states.reshape(tokens, width)
    dp, feat = lax.axis_size("dp"), lax.axis_size("feat")
    scale = 1.0 / float(tokens * dp * feat)
    blocks = dp * feat
    blk = hidden // blocks
    part = channels // feat
    orders = stage_orders(dp, feat)
    stages = log2(dp) + log2(feat)
    streams, bufs, groups = [], [], [[], [], []]
    layout = [
        (0, channels, (3, 3, 2), (0, 0, 0), (0, 1, 2)),
        (1, width, (3, 3, 2, 1), (1, 1, 2, 2), (0, 1, 0, 1)),
    ]
    for which, size, shares, group_of, order_of in layout:
        for (lo, hi), group, kind in zip(units(size, shares), group_of, order_of):
            order = orders[kind]
            split = splits(order, dp, feat)
            groups[group].append(len(streams))
            streams.append((order, split, which, lo, hi))
            bufs.append(pltpu.VMEM((split[0][0] * split[0][1], blk, hi - lo), f32))
            for above, below in split:
                bufs += [pltpu.VMEM((above * below, blk, hi - lo), bf16)] * 2
    vmem = pl.BlockSpec(memory_space=pltpu.VMEM)
    hbm = pl.BlockSpec(memory_space=pl.ANY)
    small_rows = -(-(blocks + channels // 128 + 1) // 8) * 8
    gout, gin, gsmall, ghid = pl.pallas_call(
        functools.partial(train_kernel, (groups, streams, dp, feat, blk)),
        out_shape=(
            jax.ShapeDtypeStruct((blk, channels), f32),
            jax.ShapeDtypeStruct((blk, width), f32),
            jax.ShapeDtypeStruct((small_rows, 128), f32),
            jax.ShapeDtypeStruct((tokens, width), bf16),
        ),
        in_specs=[hbm] * 4 + [vmem] * 2,
        out_specs=(vmem,) * 4,
        scratch_shapes=[
            pltpu.VMEM((tokens, width), bf16),
            pltpu.VMEM((hidden, width), bf16),
            pltpu.VMEM((hidden, channels), bf16),
            pltpu.VMEM((feat, samples, seq, part), bf16),
            pltpu.VMEM((tokens, hidden), bf16),
            pltpu.VMEM((hidden, tokens), bf16),
            pltpu.VMEM((hidden, tokens), bf16),
            pltpu.VMEM((tokens, hidden), f32),
            pltpu.VMEM((tokens, channels), f32),
            pltpu.VMEM((tokens, channels), bf16),
            pltpu.VMEM((1, hidden), f32),
            pltpu.VMEM((1, channels), f32),
            pltpu.VMEM((1, 1), f32),
        ]
        + bufs
        + [
            pltpu.VMEM((stages, small_rows, 128), f32),
            pltpu.VMEM((stages, small_rows, 128), f32),
            pltpu.SemaphoreType.DMA((len(streams) + 1, stages)),
            pltpu.SemaphoreType.DMA((len(streams) + 1, stages)),
            pltpu.SemaphoreType.DMA((feat - 1,)),
            pltpu.SemaphoreType.DMA((feat - 1,)),
            pltpu.SemaphoreType.DMA((4,)),
        ],
        compiler_params=pltpu.CompilerParams(collective_id=0, has_side_effects=True, vmem_limit_bytes=63 * 1024 * 1024),
        name="train",
    )(teacher, rows, proj_in, proj_out, bias_in.reshape(1, hidden), bias_out.reshape(1, channels))
    grad_in, grad_bias_in, grad_out, grad_bias_out, grad_hidden, loss = pl.pallas_call(
        functools.partial(place_kernel, scale, blocks),
        out_shape=(
            jax.ShapeDtypeStruct((blk, width), f32),
            jax.ShapeDtypeStruct((1, blk), f32),
            jax.ShapeDtypeStruct((blk, channels), f32),
            jax.ShapeDtypeStruct((channels // 128, 128), f32),
            jax.ShapeDtypeStruct((tokens, width), bf16),
            jax.ShapeDtypeStruct((1, 1), f32),
        ),
        in_specs=[vmem] * 4,
        out_specs=(vmem,) * 6,
        name="place",
    )(gout, gin, gsmall, ghid)
    return (
        grad_in,
        grad_bias_in.reshape(blk),
        grad_out,
        grad_bias_out.reshape(channels),
        grad_hidden.reshape(samples, seq, width),
        loss.reshape(()),
    )


def solution(mesh):
    return jax.shard_map(
        on_device,
        mesh=mesh,
        in_specs=(P(("dp", "feat"), None, None), P("dp", None, "feat"), P(), P(), P(), P()),
        out_specs=(
            P(("dp", "feat"), None),
            P(("dp", "feat")),
            P(("dp", "feat"), None),
            P(),
            P(("dp", "feat"), None, None),
            P(),
        ),
        check_vma=False,
    )
```

```python
import functools

import jax
import jax.numpy as jnp
from jax import lax
from jax.experimental import pallas as pl
from jax.experimental.pallas import tpu as pltpu
from jax.sharding import PartitionSpec as P

epsilon = 1e-06
f32 = jnp.float32
bf16 = jnp.bfloat16
MESH = pl.DeviceIdType.MESH


def log2(n):
    return n.bit_length() - 1


def stage_orders(dp, feat):
    across = [("dp", b) for b in range(1, log2(dp))]
    along = [("feat", b) for b in range(log2(feat))]
    half = len(across) // 2
    core = [("dp", 0)]
    return core + across + along, core + across[half:] + across[:half] + along, core + along + across


def splits(order, dp, feat):
    left = [("dp", b) for b in reversed(range(log2(dp)))] + [("feat", b) for b in reversed(range(log2(feat)))]
    out = []
    for bit in order:
        p = left.index(bit)
        out.append((2**p, 2 ** (len(left) - p - 1)))
        left.remove(bit)
    return out


def train_kernel(plan, teacher_hbm, rows_hbm, win_hbm, wout_hbm, bias_in, bias_out, gout, gin, gsmall, ghid,
                 rows, win, wout, tea, act, act_t, dpre_t, dsilu, out, cot, brow, bacc, lacc, *rest):
    groups, streams, dp, feat, blk = plan
    stages = log2(dp) + log2(feat)
    bufs, at = [], 0
    for _ in streams:
        bufs.append(rest[at : at + 1 + 2 * stages])
        at += 1 + 2 * stages
    small_send, small_recv, send_sem, recv_sem, tea_send, tea_recv, load_sem = rest[at:]
    place = {"dp": lax.axis_index("dp"), "feat": lax.axis_index("feat")}
    dpre = act
    tokens, hidden = act.shape
    channels, width = cot.shape[1], rows.shape[1]
    samples, seq, part = tea.shape[1:]

    def mine(bit):
        axis, b = bit
        return lax.rem(lax.div(place[axis], 2**b), 2)

    def partner(bit):
        axis, b = bit
        return {axis: place[axis] + (1 - 2 * mine(bit)) * 2**b}

    barrier = pltpu.get_barrier_semaphore()
    for b in range(log2(dp)):
        pl.semaphore_signal(barrier, inc=1, device_id=partner(("dp", b)), device_id_type=MESH)
    for r in range(1, feat):
        peer = {"feat": lax.rem(place["feat"] + r, feat)}
        pl.semaphore_signal(barrier, inc=1, device_id=peer, device_id_type=MESH)

    loads = [
        pltpu.make_async_copy(rows_hbm, rows, load_sem.at[0]),
        pltpu.make_async_copy(win_hbm, win, load_sem.at[1]),
        pltpu.make_async_copy(wout_hbm, wout, load_sem.at[2]),
        pltpu.make_async_copy(
            teacher_hbm.at[pl.ds(place["feat"] * samples, samples)], tea.at[place["feat"]], load_sem.at[3]
        ),
    ]
    for load in loads:
        load.start()
    pl.semaphore_wait(barrier, log2(dp) + feat - 1)

    def tea_copy(sample, r):
        peer = lax.rem(place["feat"] + r, feat)
        return pltpu.make_async_remote_copy(
            src_ref=teacher_hbm.at[peer * samples + sample], dst_ref=tea.at[place["feat"], sample],
            send_sem=tea_send.at[sample, r - 1], recv_sem=tea_recv.at[sample, r - 1],
            device_id={"feat": peer}, device_id_type=MESH,
        )

    for sample in range(samples):
        for r in range(1, feat):
            tea_copy(sample, r).start()

    def copy(s, k):
        send, recv = bufs[s][1 + 2 * k : 3 + 2 * k]
        return pltpu.make_async_remote_copy(
            src_ref=send, dst_ref=recv, send_sem=send_sem.at[s, k], recv_sem=recv_sem.at[s, k],
            device_id=partner(streams[s][0][k]), device_id_type=MESH,
        )

    def small_copy(k):
        return pltpu.make_async_remote_copy(
            src_ref=small_send.at[k], dst_ref=small_recv.at[k],
            send_sem=send_sem.at[len(streams), k], recv_sem=recv_sem.at[len(streams), k],
            device_id=partner(streams[0][0][k]), device_id_type=MESH,
        )

    wide = 256

    def first_map(j, _):
        cut = pl.ds(pl.multiple_of(j * wide, wide), wide)
        pre = lax.dot_general(rows[...], win[cut, :], (((1,), (1,)), ((), ())), preferred_element_type=f32)
        pre = pre + bias_in[:, cut]
        sig = jax.nn.sigmoid(pre)
        got = (pre * sig).astype(bf16)
        act[:, cut] = got
        act_t[cut, :] = got.T
        dsilu[:, cut] = sig * (1.0 + pre * (1.0 - sig))
        return 0

    def last_map(j, _):
        cut = pl.ds(pl.multiple_of(j * wide, wide), wide)
        out[:, cut] = jnp.dot(act[...], wout[:, cut], preferred_element_type=f32) + bias_out[:, cut]
        return 0

    some = 64

    def cotangent(sample, i, loss):
        at = pl.ds(pl.multiple_of(sample * seq + i * some, some), some)
        inner = pl.ds(pl.multiple_of(i * some, some), some)
        zz = jnp.zeros((some, 1), f32)
        yy, zy = zz, zz
        for c in range(feat):
            o = out[at, c * part : (c + 1) * part]
            t = tea[c, sample, inner, :].astype(f32)
            zz = zz + jnp.sum(o * o, axis=1, keepdims=True)
            yy = yy + jnp.sum(t * t, axis=1, keepdims=True)
            zy = zy + jnp.sum(o * t, axis=1, keepdims=True)
        norm_z = jnp.sqrt(zz + epsilon)
        norm_y = jnp.sqrt(yy + epsilon)
        inverse = 1.0 / (norm_z * norm_y)
        cosine = zy * inverse
        weight = cosine / (norm_z * norm_z)
        for c in range(feat):
            o = out[at, c * part : (c + 1) * part]
            t = tea[c, sample, inner, :].astype(f32)
            got = (weight * o - t * inverse).astype(bf16)
            cot[at, c * part : (c + 1) * part] = got
            bacc[:, c * part : (c + 1) * part] += jnp.sum(got.astype(f32), axis=0, keepdims=True)
        return loss + jnp.sum(cosine, axis=0, keepdims=True)

    def backward(sample, j, _):
        cut = pl.ds(pl.multiple_of(j * wide, wide), wide)
        own = slice(sample * seq, (sample + 1) * seq)
        back = lax.dot_general(cot[own, :], wout[cut, :], (((1,), (1,)), ((), ())), preferred_element_type=f32)
        got = (back * dsilu[own, cut]).astype(bf16)
        dpre[own, cut] = got
        dpre_t[cut, own] = got.T
        brow[:, cut] += jnp.sum(got.astype(f32), axis=0, keepdims=True)
        return 0

    def back_through(sample):
        lax.fori_loop(0, hidden // wide, functools.partial(backward, sample), 0)

    step = 384 if width % 384 == 0 else 128

    def to_rows(j, _):
        cut = pl.ds(pl.multiple_of(j * step, step), step)
        ghid[:, cut] = jnp.dot(dpre[...], win[:, cut], preferred_element_type=f32).astype(bf16)
        return 0

    def produce(s, sends):
        order, split, which, lo_col, hi_col = streams[s]
        lhs, rhs = (act_t, cot) if which == 0 else (dpre_t, rows)
        hi, lo = split[0]
        keep, send, recv = bufs[s][:3]
        own = mine(order[0])

        def term(h, bit):
            at = pl.multiple_of((h * 2 + bit) * (lo * blk), lo * blk)
            got = jnp.dot(lhs[pl.ds(at, lo * blk), :], rhs[:, lo_col:hi_col], preferred_element_type=f32)
            return got.reshape(lo, blk, hi_col - lo_col)

        def to_send(h, _):
            send[pl.ds(h * lo, lo)] = term(h, 1 - own).astype(bf16)
            return 0

        def to_keep(h, _):
            keep[pl.ds(h * lo, lo)] = term(h, own)
            return 0

        if sends:
            lax.fori_loop(0, hi, to_send, 0)
            copy(s, 0).start()
        else:
            lax.fori_loop(0, hi, to_keep, 0)

    def produce_all(group):
        for s in group:
            produce(s, True)
        for s in group:
            produce(s, False)

    def advance(s, k):
        order, split = streams[s][:2]
        hi, lo = split[k]
        keep, recv0, send = bufs[s][0], bufs[s][2 * k], bufs[s][2 * k + 1]
        own = mine(order[k])
        copy(s, k - 1).wait_recv()

        def total(i, bit):
            at = (lax.div(i, lo) * 2 + bit) * lo + lax.rem(i, lo)
            return keep[at] + recv0[at].astype(f32)

        def to_send(i, _):
            send[i] = total(i, 1 - own).astype(bf16)
            return 0

        def to_keep(i, _):
            keep[i] = total(i, own)
            return 0

        lax.fori_loop(0, hi * lo, to_send, 0)
        copy(s, k).start()
        lax.fori_loop(0, hi * lo, to_keep, 0)

    blocks = dp * feat

    def small_step(k):
        if k == 0:
            small_send[0] = jnp.zeros(small_send.shape[1:], f32)
            for j in range(blocks):
                small_send[0, j : j + 1, 0:blk] = brow[:, j * blk : (j + 1) * blk]
            for j in range(channels // 128):
                small_send[0, blocks + j : blocks + j + 1, :] = bacc[:, j * 128 : (j + 1) * 128]
            last = blocks + channels // 128
            small_send[0, last : last + 1, :] = jnp.broadcast_to(lacc[...], (1, 128))
        else:
            small_copy(k - 1).wait_recv()
            small_send[k] = small_send[k - 1] + small_recv[k - 1]
        small_copy(k).start()

    def finish(s):
        which, lo_col, hi_col = streams[s][2:]
        copy(s, stages - 1).wait_recv()
        target = gout if which == 0 else gin
        target[:, lo_col:hi_col] = bufs[s][0][0] + bufs[s][2 * stages][0].astype(f32)

    loads[0].wait()
    loads[1].wait()
    lax.fori_loop(0, hidden // wide, first_map, 0)
    loads[2].wait()
    lax.fori_loop(0, channels // wide, last_map, 0)
    bacc[...] = jnp.zeros_like(bacc)
    brow[...] = jnp.zeros_like(brow)
    loads[3].wait()
    loss = jnp.zeros((1, 1), f32)
    for sample in range(samples):
        for r in range(1, feat):
            tea_copy(sample, r).wait_recv()
        loss = lax.fori_loop(0, seq // some, functools.partial(cotangent, sample), loss)
        if sample < samples - 1:
            back_through(sample)
    lacc[...] = loss

    first, second, third = groups
    one, two, other = first
    produce(one, True)
    produce(two, True)
    produce(one, False)
    produce(other, True)
    advance(one, 1)
    produce(two, False)
    advance(two, 1)
    produce(other, False)
    advance(other, 1)
    back_through(samples - 1)
    produce_all(second)
    small_step(0)
    for s in second:
        advance(s, 1)
    small_step(1)
    produce_all(third)
    for s in first:
        advance(s, 2)
    lax.fori_loop(0, width // step, to_rows, 0)
    for t in range(3, stages + 3):
        for g in (2, 1, 0):
            k = t - g
            for s in groups[g]:
                if k < stages:
                    advance(s, k)
                elif k == stages:
                    finish(s)
            if g == 1 and k < stages:
                small_step(k)
    small_copy(stages - 1).wait_recv()
    gsmall[...] = small_send[stages - 1] + small_recv[stages - 1]
    for sample in range(samples):
        for r in range(1, feat):
            tea_copy(sample, r).wait_send()
    for k in range(stages):
        for s in range(len(streams)):
            copy(s, k).wait_send()
        small_copy(k).wait_send()


def place_kernel(scale, blocks, gout, gin, gsmall, ghid, out_in, out_bias_in, out_out, out_bias_out, out_hid, out_loss):
    me = lax.axis_index("dp") * lax.axis_size("feat") + lax.axis_index("feat")
    out_in[...] = gin[...] * scale
    out_out[...] = gout[...] * scale
    out_hid[...] = ghid[...]
    blk = out_bias_in.shape[1]
    out_bias_in[...] = gsmall[pl.ds(me, 1), 0:blk] * scale
    rows = out_bias_out.shape[0]
    out_bias_out[...] = gsmall[blocks : blocks + rows, :] * scale
    out_loss[...] = gsmall[blocks + rows : blocks + rows + 1, 0:1] * (-scale)


def units(size, shares):
    total, parts, edge = size // 128, [], 0
    for i in range(len(shares)):
        upto = round(total * sum(shares[: i + 1]) / sum(shares))
        parts.append((edge * 128, upto * 128 if i < len(shares) - 1 else size))
        edge = upto
    return parts


def on_device(hidden_states, teacher, proj_in, bias_in, proj_out, bias_out):
    samples, seq, width = hidden_states.shape
    hidden, channels = proj_out.shape
    tokens = samples * seq
    rows = hidden_states.reshape(tokens, width)
    dp, feat = lax.axis_size("dp"), lax.axis_size("feat")
    scale = 1.0 / float(tokens * dp * feat)
    blocks = dp * feat
    blk = hidden // blocks
    part = channels // feat
    orders = stage_orders(dp, feat)
    stages = log2(dp) + log2(feat)
    streams, bufs, groups = [], [], [[], [], []]
    layout = [
        (0, channels, (3, 3, 2), (0, 0, 0), (0, 1, 2)),
        (1, width, (3, 3, 2, 1), (1, 1, 2, 2), (0, 1, 0, 1)),
    ]
    for which, size, shares, group_of, order_of in layout:
        for (lo, hi), group, kind in zip(units(size, shares), group_of, order_of):
            order = orders[kind]
            split = splits(order, dp, feat)
            groups[group].append(len(streams))
            streams.append((order, split, which, lo, hi))
            bufs.append(pltpu.VMEM((split[0][0] * split[0][1], blk, hi - lo), f32))
            for above, below in split:
                bufs += [pltpu.VMEM((above * below, blk, hi - lo), bf16)] * 2
    vmem = pl.BlockSpec(memory_space=pltpu.VMEM)
    hbm = pl.BlockSpec(memory_space=pl.ANY)
    small_rows = -(-(blocks + channels // 128 + 1) // 8) * 8
    gout, gin, gsmall, ghid = pl.pallas_call(
        functools.partial(train_kernel, (groups, streams, dp, feat, blk)),
        out_shape=(
            jax.ShapeDtypeStruct((blk, channels), f32),
            jax.ShapeDtypeStruct((blk, width), f32),
            jax.ShapeDtypeStruct((small_rows, 128), f32),
            jax.ShapeDtypeStruct((tokens, width), bf16),
        ),
        in_specs=[hbm] * 4 + [vmem] * 2,
        out_specs=(vmem,) * 4,
        scratch_shapes=[
            pltpu.VMEM((tokens, width), bf16),
            pltpu.VMEM((hidden, width), bf16),
            pltpu.VMEM((hidden, channels), bf16),
            pltpu.VMEM((feat, samples, seq, part), bf16),
            pltpu.VMEM((tokens, hidden), bf16),
            pltpu.VMEM((hidden, tokens), bf16),
            pltpu.VMEM((hidden, tokens), bf16),
            pltpu.VMEM((tokens, hidden), f32),
            pltpu.VMEM((tokens, channels), f32),
            pltpu.VMEM((tokens, channels), bf16),
            pltpu.VMEM((1, hidden), f32),
            pltpu.VMEM((1, channels), f32),
            pltpu.VMEM((1, 1), f32),
        ]
        + bufs
        + [
            pltpu.VMEM((stages, small_rows, 128), f32),
            pltpu.VMEM((stages, small_rows, 128), f32),
            pltpu.SemaphoreType.DMA((len(streams) + 1, stages)),
            pltpu.SemaphoreType.DMA((len(streams) + 1, stages)),
            pltpu.SemaphoreType.DMA((samples, feat - 1)),
            pltpu.SemaphoreType.DMA((samples, feat - 1)),
            pltpu.SemaphoreType.DMA((4,)),
        ],
        compiler_params=pltpu.CompilerParams(collective_id=0, has_side_effects=True, vmem_limit_bytes=63 * 1024 * 1024),
        name="train",
    )(teacher, rows, proj_in, proj_out, bias_in.reshape(1, hidden), bias_out.reshape(1, channels))
    grad_in, grad_bias_in, grad_out, grad_bias_out, grad_hidden, loss = pl.pallas_call(
        functools.partial(place_kernel, scale, blocks),
        out_shape=(
            jax.ShapeDtypeStruct((blk, width), f32),
            jax.ShapeDtypeStruct((1, blk), f32),
            jax.ShapeDtypeStruct((blk, channels), f32),
            jax.ShapeDtypeStruct((channels // 128, 128), f32),
            jax.ShapeDtypeStruct((tokens, width), bf16),
            jax.ShapeDtypeStruct((1, 1), f32),
        ),
        in_specs=[vmem] * 4,
        out_specs=(vmem,) * 6,
        name="place",
    )(gout, gin, gsmall, ghid)
    return (
        grad_in,
        grad_bias_in.reshape(blk),
        grad_out,
        grad_bias_out.reshape(channels),
        grad_hidden.reshape(samples, seq, width),
        loss.reshape(()),
    )


def solution(mesh):
    return jax.shard_map(
        on_device,
        mesh=mesh,
        in_specs=(P(("dp", "feat"), None, None), P("dp", None, "feat"), P(), P(), P(), P()),
        out_specs=(
            P(("dp", "feat"), None),
            P(("dp", "feat")),
            P(("dp", "feat"), None),
            P(),
            P(("dp", "feat"), None, None),
            P(),
        ),
        check_vma=False,
    )
```
